32 devices in a mesh: dp: 1 (over z), cols: 4 (over y), rows: 8 (over x, core).
Axes of the slice: x: 4, y: 4, z: 1, core: 2. Of those that a mesh axis runs over, the one named last changes fastest.
The devices are a block of a 4x4x8 slice.
Arguments:
- frames: bfloat16 [32, 1, 512, 256, 4], P(None, 'dp', 'rows', 'cols')
- w_in: bfloat16 [3, 3, 4, 256], replicated
- w_rec: bfloat16 [3, 3, 64, 256], replicated
- gate_bias: float32 [256], replicated
- h_init: bfloat16 [1, 512, 256, 64], P('dp', 'rows', 'cols')
- c_init: float32 [1, 512, 256, 64], P('dp', 'rows', 'cols')
Outputs:
- output 1: bfloat16 [32, 1, 512, 256, 64], P(None, 'dp', 'rows', 'cols')
- output 2: float32 [1, 512, 256, 64], P('dp', 'rows', 'cols')
All inputs are finite; a program needn't handle non-finite values.
Results may differ from the reference program's by a relative error of at most 0.00442392.
Values are sent between devices in bfloat16 or wider.
A program may use at most 768 MiB of HBM per device.

```python
import jax
import jax.numpy as jnp
from jax import lax

STEPS = 32
BATCH = 1
GRID_H = 512
GRID_W = 256
C_IN = 4
C_HID = 64

CONV_DIMS = ("NHWC", "HWIO", "NHWC")


def setup_inputs(seed: int = 0, part: int = 0) -> dict:
    part_key = jax.random.fold_in(jax.random.key(seed), part)
    k_frames, k_hid, k_cell = jax.random.split(part_key, 3)
    k_win, k_wrec, k_bias = jax.random.split(jax.random.key(seed + 1), 3)
    frames = jax.random.normal(k_frames, (STEPS, BATCH, GRID_H, GRID_W, C_IN), jnp.float32)
    w_in = jax.random.normal(k_win, (3, 3, C_IN, 4 * C_HID), jnp.float32) * (9 * C_IN) ** -0.5
    w_rec = jax.random.normal(k_wrec, (3, 3, C_HID, 4 * C_HID), jnp.float32) * (2.0 * (9 * C_HID) ** -0.5)
    forget_shift = jnp.concatenate([jnp.zeros((C_HID,), jnp.float32), jnp.ones((C_HID,), jnp.float32), jnp.zeros((2 * C_HID,), jnp.float32)])
    gate_bias = 0.5 * jax.random.normal(k_bias, (4 * C_HID,), jnp.float32) + forget_shift
    h_init = 0.5 * jax.random.normal(k_hid, (BATCH, GRID_H, GRID_W, C_HID), jnp.float32)
    c_init = jax.random.normal(k_cell, (BATCH, GRID_H, GRID_W, C_HID), jnp.float32)
    return {
        "frames": frames.astype(jnp.bfloat16),
        "w_in": w_in.astype(jnp.bfloat16),
        "w_rec": w_rec.astype(jnp.bfloat16),
        "gate_bias": gate_bias,
        "h_init": h_init.astype(jnp.bfloat16),
        "c_init": c_init,
    }


def conv_same(operand, kernel):
    return lax.conv_general_dilated(operand.astype(jnp.float32), kernel, (1, 1), "SAME", dimension_numbers=CONV_DIMS)


def reference(frames, w_in, w_rec, gate_bias, h_init, c_init):
    w_in32 = w_in.astype(jnp.float32)
    w_rec32 = w_rec.astype(jnp.float32)

    def time_step(carry_in, frame_t):
        h_prev, c_prev = carry_in
        gate_pre = conv_same(frame_t, w_in32) + conv_same(h_prev, w_rec32) + gate_bias
        gate_i, gate_f, gate_o, gate_g = jnp.split(gate_pre, 4, axis=-1)
        c_next = jax.nn.sigmoid(gate_f) * c_prev + jax.nn.sigmoid(gate_i) * jnp.tanh(gate_g)
        h_next = (jax.nn.sigmoid(gate_o) * jnp.tanh(c_next)).astype(jnp.bfloat16)
        return (h_next, c_next), h_next

    (h_last, c_last), hidden_seq = lax.scan(time_step, (h_init, c_init), frames)
    return hidden_seq, c_last
```

```python
import functools

import jax
import jax.numpy as jnp
from jax import lax
from jax.experimental import pallas as pl
from jax.experimental.pallas import tpu as pltpu
from jax.sharding import PartitionSpec as P

MESH = pl.DeviceIdType.MESH
BF16, F32 = jnp.bfloat16, jnp.float32
LANES = 128


def chunk_order(n):
    order = [0]
    low, high = 1, n - 1
    while low <= high:
        order.append(low)
        if high != low:
            order.append(high)
        low, high = low + 1, high - 1
    return order


def cell_kernel(cfg, fr_ref, w_ref, bias_ref, h0_ref, c0_ref, mask_ref, out_ref, c_ref,
                ha, hb, left_a, left_b, right_a, right_b, gates,
                col_out, col_in, row_out, row_in, diag_in,
                col_ssem, col_rsem, row_ssem, row_rsem, diag_ssem, diag_rsem, out_sem):
    steps, half, chan, n_chunks, n_rows, n_cols = cfg
    per = half // n_chunks
    groups = chan // 16
    order = chunk_order(n_chunks)
    first, last = 0, n_chunks - 1
    my_row, my_col = lax.axis_index("rows"), lax.axis_index("cols")
    has_up, has_down = my_row > 0, my_row < n_rows - 1
    has_left, has_right = my_col > 0, my_col < n_cols - 1
    h_refs, l_refs, r_refs = (ha, hb), (left_a, left_b), (right_a, right_b)

    def mask(index):
        return mask_ref[index] > 0

    even, low_half = mask(0), mask(1)
    lane_first, lane_last = mask(2), mask(3)

    def copy(src, dst, ssem, rsem, drow, dcol):
        return pltpu.make_async_remote_copy(src_ref=src, dst_ref=dst, send_sem=ssem, recv_sem=rsem,
                                            device_id={"rows": my_row + drow, "cols": my_col + dcol}, device_id_type=MESH)

    def col_copy(par, side, chunk):
        return copy(col_out.at[par, side, chunk], col_in.at[par, side, chunk], col_ssem.at[par, side, chunk],
                    col_rsem.at[par, side, chunk], 0, 1 if side == 0 else -1)

    def row_copy(par, side):
        return copy(row_out.at[par, side], row_in.at[par, side], row_ssem.at[par, side], row_rsem.at[par, side],
                    1 if side == 0 else -1, 0)

    def diag_copy(par, slot):
        chunk = last if slot < 2 else first
        return copy(col_out.at[par, slot % 2, chunk], diag_in.at[par, slot], diag_ssem.at[par, slot],
                    diag_rsem.at[par, slot], 1 if slot < 2 else -1, 1 if slot % 2 == 0 else -1)

    col_to, col_from = (has_right, has_left), (has_left, has_right)
    row_to, row_from = (has_down, has_up), (has_up, has_down)
    diag_to = tuple((has_down if s < 2 else has_up) & col_to[s % 2] for s in range(4))
    diag_from = tuple((has_up if s < 2 else has_down) & col_from[s % 2] for s in range(4))

    def start_chunk(par, chunk, live):
        for side in range(2):
            @pl.when(col_to[side] & live)
            def _():
                col_copy(par, side, chunk).start()
        if chunk in (first, last):
            side = 0 if chunk == last else 1

            @pl.when(row_to[side] & live)
            def _():
                row_copy(par, side).start()
            for slot in ((0, 1) if chunk == last else (2, 3)):
                @pl.when(diag_to[slot] & live)
                def _():
                    diag_copy(par, slot).start()

    def wait_for(par, chunks, edge):
        for side in range(2):
            if chunks:
                @pl.when(col_from[side])
                def _():
                    for chunk in chunks:
                        col_copy(par, side, chunk).wait_recv()
                        col_copy(par, 1 - side, chunk).wait_send()
        if edge is not None:
            side = 0 if edge == first else 1

            @pl.when(row_from[side])
            def _():
                row_copy(par, side).wait_recv()
                row_copy(par, 1 - side).wait_send()
            for slot in ((0, 1) if edge == first else (2, 3)):
                @pl.when(diag_from[slot])
                def _():
                    diag_copy(par, slot).wait_recv()
                    diag_copy(par, 3 - slot).wait_send()

    def shifted(par, row, message, rolls):
        for g in range(groups):
            place = pl.ds(row * chan + 16 * g, 16)
            cells = h_refs[par][place, :]
            halo = pltpu.roll(message, rolls[g] % LANES, 1)
            l_refs[par][place, :] = jnp.where(lane_first, halo, pltpu.roll(cells, 1, 1))
            r_refs[par][place, :] = jnp.where(lane_last, halo, pltpu.roll(cells, LANES - 1, 1))

    def col_message(par, chunk):
        return jnp.where(even, col_in[par, 0, chunk], col_in[par, 1, chunk])

    def patch(par, chunks, edge):
        for chunk in chunks:
            message = col_message(par, chunk)
            for q in range(per):
                shifted(par, chunk * per + q + 1, message, [-2 * (q * groups + g) for g in range(groups)])
        if edge is not None:
            side = 0 if edge == first else 1
            diag = jnp.where(even, diag_in[par, 2 * side], diag_in[par, 2 * side + 1])
            other = last if edge == first else first
            q = per - 1 if edge == first else 0
            row = 0 if edge == first else half + 1
            for g in range(groups):
                place = slice(16 * g, 16 * (g + 1))
                mine, theirs = row_out[par, side, place, :], row_in[par, side, place, :]
                joined = jnp.where(low_half, theirs, mine) if edge == first else jnp.where(low_half, mine, theirs)
                h_refs[par][pl.ds(row * chan + 16 * g, 16), :] = joined
            message = jnp.where(mask(4 + side), diag, col_message(par, other))
            shifted(par, row, message, [64 - 2 * (q * groups + g) for g in range(groups)])

    def publish(par, chunk):
        parts = [h_refs[par][pl.ds((chunk * per + s // groups + 1) * chan + 16 * (s % groups), 16), :]
                 for s in range(per * groups)]
        level = 0
        while len(parts) > 1:
            keep = mask(6 + level)
            parts = [jnp.where(keep, parts[2 * i], pltpu.roll(parts[2 * i + 1], 2 << level, 1)) for i in range(len(parts) // 2)]
            level += 1
        col_out[par, 0, chunk] = pltpu.roll(parts[0], 65, 1)
        col_out[par, 1, chunk] = pltpu.roll(parts[0], 63, 1)
        if chunk in (first, last):
            side = 0 if chunk == last else 1
            row = half if chunk == last else 1
            for g in range(groups):
                row_out[par, side, 16 * g:16 * (g + 1), :] = pltpu.roll(h_refs[par][pl.ds(row * chan + 16 * g, 16), :], 64, 1)

    def multiply(par, t, chunk, slot):
        blocks = []
        for q in range(per):
            place = pl.ds((chunk * per + q) * chan, 3 * chan)
            frame = fr_ref[t, pl.ds((chunk * per + q) * 16, 48), :]
            blocks.append(jnp.concatenate([l_refs[par][place, :], h_refs[par][place, :], r_refs[par][place, :], frame], axis=0))
        gates[slot] = jnp.dot(w_ref[...], jnp.concatenate(blocks, axis=1), preferred_element_type=F32)

    def sigmoid(x):
        return 0.5 * jnp.tanh(0.5 * x) + 0.5

    def update(par, chunk, slot):
        for q in range(per):
            pre = [gates[slot, pl.ds(b * chan, chan), q * LANES:(q + 1) * LANES] + bias_ref[pl.ds(b * chan, chan), :]
                   for b in range(4)]
            place = pl.ds((chunk * per + q) * chan, chan)
            c_next = sigmoid(pre[1]) * c_ref[place, :] + sigmoid(pre[0]) * jnp.tanh(pre[3])
            c_ref[place, :] = c_next
            h_refs[par][pl.ds((chunk * per + q + 1) * chan, chan), :] = (sigmoid(pre[2]) * jnp.tanh(c_next)).astype(BF16)

    def out_copy(par, t):
        return pltpu.make_async_copy(h_refs[par].at[pl.ds(chan, half * chan), :], out_ref.at[t], out_sem.at[par])

    needs, seen = [], set()
    for chunk in order:
        chunks, edge = [], None
        for near in (chunk - 1, chunk, chunk + 1):
            if 0 <= near < n_chunks and near not in seen:
                seen.add(near)
                chunks.append(near)
        if chunk in (first, last):
            edge = chunk
        needs.append((chunks, edge))
    waits, waited = [], set()
    for chunks, edge in needs:
        group = list(chunks)
        if edge is not None:
            group.append(last if edge == first else first)
        group = [c for c in group if c not in waited]
        waited.update(group)
        waits.append((group, edge))

    for par in range(2):
        col_in[par] = jnp.zeros(col_in.shape[1:], BF16)
        row_in[par] = jnp.zeros(row_in.shape[1:], BF16)
        diag_in[par] = jnp.zeros(diag_in.shape[1:], BF16)
    barrier = pltpu.get_barrier_semaphore()
    count = jnp.int32(0)
    for drow in (-1, 0, 1):
        for dcol in (-1, 0, 1):
            if (drow, dcol) == (0, 0):
                continue
            there = jnp.bool_(True)
            if drow:
                there = there & (has_down if drow > 0 else has_up)
            if dcol:
                there = there & (has_right if dcol > 0 else has_left)

            @pl.when(there)
            def _():
                pl.semaphore_signal(barrier, inc=1, device_id={"rows": my_row + drow, "cols": my_col + dcol}, device_id_type=MESH)
            count = count + there.astype(jnp.int32)
    pl.semaphore_wait(barrier, count)

    c_ref[...] = c0_ref[...]
    ha[pl.ds(chan, half * chan), :] = h0_ref[...]
    for chunk in order:
        publish(0, chunk)
        start_chunk(0, chunk, True)

    def step(t, par, old):
        live = t < steps - 1

        @pl.when(old)
        def _():
            out_copy(1 - par, t - 2).wait()
        wait_for(par, *waits[0])
        patch(par, *needs[0])
        for i, chunk in enumerate(order):
            if i + 1 < n_chunks:
                wait_for(par, *waits[i + 1])
            multiply(par, t, chunk, i % 2)
            if i + 1 < n_chunks:
                patch(par, *needs[i + 1])
            if i > 0:
                update(1 - par, order[i - 1], (i - 1) % 2)
                publish(1 - par, order[i - 1])
                start_chunk(1 - par, order[i - 1], live)
        update(1 - par, order[-1], (n_chunks - 1) % 2)
        publish(1 - par, order[-1])
        start_chunk(1 - par, order[-1], live)
        out_copy(1 - par, t).start()

    def two_steps(i, carry):
        step(2 * i, 0, i > 0)
        step(2 * i + 1, 1, i > 0)
        return carry

    lax.fori_loop(0, steps // 2, two_steps, 0)
    out_copy(1, steps - 2).wait()
    out_copy(0, steps - 1).wait()


def lane_masks(per, groups):
    lane = jnp.arange(LANES)
    slots = per * groups
    corner = jnp.isin(lane, jnp.array([0, 63, 64, 127]))
    top = (2 * ((per - 1) * groups + jnp.arange(groups)))
    low = 2 * jnp.arange(groups)
    rows = [lane % 2 == 0, lane < 64, lane % 64 == 0, lane % 64 == 63,
            jnp.isin(lane, jnp.concatenate([top + 64, (top - 1) % LANES])),
            jnp.isin(lane, jnp.concatenate([low, low + 63]))]
    keep = corner
    level = 0
    while (1 << level) < slots:
        rows.append(keep)
        keep = keep | jnp.roll(keep, 2 << level)
        level += 1
    return jnp.broadcast_to(jnp.stack(rows)[:, None, :], (len(rows), 16, LANES)).astype(BF16)


def untile_kernel(x_ref, o_ref):
    half, chan = o_ref.shape[1] // 2, o_ref.shape[3]
    for k in range(half):
        cells = x_ref[0, pl.ds(k * chan, chan), :].T
        o_ref[0, k] = cells[:64]
        o_ref[0, k + half] = cells[64:]


def edge_exchange(tile_in, axis_name, axis_size, axis_dim):
    length = tile_in.shape[axis_dim]
    low_part = lax.slice_in_dim(tile_in, 0, 1, axis=axis_dim)
    high_part = lax.slice_in_dim(tile_in, length - 1, length, axis=axis_dim)
    if axis_size == 1:
        from_prev, from_next = jnp.zeros_like(high_part), jnp.zeros_like(low_part)
    else:
        forward = [(source, source + 1) for source in range(axis_size - 1)]
        backward = [(source + 1, source) for source in range(axis_size - 1)]
        from_prev = lax.ppermute(high_part, axis_name, forward)
        from_next = lax.ppermute(low_part, axis_name, backward)
    return jnp.concatenate([from_prev, tile_in, from_next], axis=axis_dim)


N_CHUNKS = 8


def solution(mesh):
    n_rows, n_cols = mesh.shape["rows"], mesh.shape["cols"]
    seq_spec = P(None, "dp", "rows", "cols", None)
    state_spec = P("dp", "rows", "cols", None)

    def local_run(frames, w_in, w_rec, gate_bias, h_init, c_init):
        steps, batch, height, width, c_in = frames.shape
        chan = h_init.shape[-1]
        half = height // 2
        assert batch == 1 and width == 64 and chan == 64 and c_in == 4 and steps % 2 == 0
        per, groups = half // N_CHUNKS, chan // 16

        def to_lanes(state):
            parts = state[0].reshape(2, half, width, chan).transpose(1, 3, 0, 2)
            return parts.reshape(half * chan, 2 * width)

        flat = frames[:, 0].transpose(0, 1, 3, 2)
        flat = edge_exchange(flat, "rows", n_rows, 1)
        flat = edge_exchange(flat, "cols", n_cols, 3)
        flat = jnp.stack([flat[..., dx:dx + width] for dx in range(3)], axis=2).reshape(steps, height + 2, 3 * c_in, width)
        flat = jnp.pad(flat, ((0, 0), (0, 0), (0, 16 - 3 * c_in), (0, 0)))
        flat = jnp.concatenate([flat[:, :half + 2], flat[:, half:]], axis=3).reshape(steps, (half + 2) * 16, LANES)

        gates_n = w_rec.shape[-1]
        w_h = w_rec.transpose(1, 0, 2, 3).reshape(9 * chan, gates_n)
        w_x = jnp.pad(w_in.reshape(3, 3 * c_in, gates_n), ((0, 0), (0, 16 - 3 * c_in), (0, 0))).reshape(48, gates_n)
        weights = jnp.concatenate([w_h, w_x], axis=0).T
        bias = jnp.broadcast_to(gate_bias[:, None], (gates_n, LANES))

        vmem = pl.BlockSpec(memory_space=pltpu.VMEM)
        cells = pltpu.VMEM(((half + 2) * chan, LANES), BF16)
        dma = pltpu.SemaphoreType.DMA
        cfg = (steps, half, chan, N_CHUNKS, n_rows, n_cols)
        hidden, c_last = pl.pallas_call(
            functools.partial(cell_kernel, cfg),
            out_shape=(jax.ShapeDtypeStruct((steps, half * chan, LANES), BF16), jax.ShapeDtypeStruct((half * chan, LANES), F32)),
            in_specs=[vmem] * 6,
            out_specs=(pl.BlockSpec(memory_space=pl.ANY), vmem),
            scratch_shapes=[cells] * 6 + [
                pltpu.VMEM((2, gates_n, per * LANES), F32),
                pltpu.VMEM((2, 2, N_CHUNKS, 16, LANES), BF16), pltpu.VMEM((2, 2, N_CHUNKS, 16, LANES), BF16),
                pltpu.VMEM((2, 2, chan, LANES), BF16), pltpu.VMEM((2, 2, chan, LANES), BF16),
                pltpu.VMEM((2, 4, 16, LANES), BF16),
                dma((2, 2, N_CHUNKS)), dma((2, 2, N_CHUNKS)), dma((2, 2)), dma((2, 2)), dma((2, 4)), dma((2, 4)), dma((2,)),
            ],
            compiler_params=pltpu.CompilerParams(collective_id=0, has_side_effects=True, vmem_limit_bytes=40 * 1024 * 1024),
        )(flat, weights, bias, to_lanes(h_init), to_lanes(c_init), lane_masks(per, groups))

        hidden_seq = pl.pallas_call(
            untile_kernel,
            out_shape=jax.ShapeDtypeStruct((steps, height, width, chan), BF16),
            grid=(steps,),
            in_specs=[pl.BlockSpec((1, half * chan, LANES), lambda t: (t, 0, 0))],
            out_specs=pl.BlockSpec((1, height, width, chan), lambda t: (t, 0, 0, 0)),
        )(hidden)
        c_last = c_last.reshape(half, chan, 2, width).transpose(2, 0, 3, 1).reshape(1, height, width, chan)
        return hidden_seq[:, None], c_last

    return jax.shard_map(local_run, mesh=mesh, in_specs=(seq_spec, P(), P(), P(), state_spec, state_spec),
                         out_specs=(seq_spec, state_spec), check_vma=False)
```

```python
import functools

import jax
import jax.numpy as jnp
import numpy as np
from jax import lax
from jax.experimental import pallas as pl
from jax.experimental.pallas import tpu as pltpu
from jax.sharding import PartitionSpec as P

MESH = pl.DeviceIdType.MESH
BF16, F32 = jnp.bfloat16, jnp.float32
LANES = 128


def chunk_order(n):
    order = [0]
    low, high = 1, n - 1
    while low <= high:
        order.append(low)
        if high != low:
            order.append(high)
        low, high = low + 1, high - 1
    return order


def cell_kernel(cfg, fr_ref, w_ref, bias_ref, h0_ref, c0_ref, mask_ref, out_ref, c_out_ref,
                ha, hb, left_a, left_b, right_a, right_b, gates, c_ref, f_mid, f_left, f_right,
                f_col_out, f_col_in, f_row_out, f_row_in, f_diag_in, f_ssem, f_rsem,
                pieces, col_out, col_in, row_out, row_in, diag_in,
                col_ssem, col_rsem, row_ssem, row_rsem, diag_ssem, diag_rsem, out_sem):
    steps, half, chan, n_chunks, n_rows, n_cols = cfg
    per = half // n_chunks
    groups = chan // 16
    order = chunk_order(n_chunks)
    first, last = 0, n_chunks - 1
    slots = per * groups
    sizes = [size for group in GROUPS for size in group]
    ends = [sum(sizes[:i + 1]) for i in range(len(sizes))]
    home = {chunk: next(card for card, end in enumerate(ends) if place < end) for place, chunk in enumerate(order)}
    base = {chunk: slots * (place - ends[home[chunk]] + sizes[home[chunk]]) for place, chunk in enumerate(order)}
    members = [[chunk for chunk in order if home[chunk] == card] for card in range(len(sizes))]
    card_from = [sum(len(group) for group in GROUPS[:i]) for i in range(len(GROUPS) + 1)]
    group_of = {chunk: max(g for g in range(len(GROUPS)) if card_from[g] <= home[chunk]) for chunk in order}
    closing = {[chunk for chunk in order if group_of[chunk] == g][-1]: g for g in range(len(GROUPS))}
    assert sum(sizes) == n_chunks and max(sizes) * slots <= 32 and home[first] == home[last] == 0
    my_row, my_col = lax.axis_index("rows"), lax.axis_index("cols")
    has_up, has_down = my_row > 0, my_row < n_rows - 1
    has_left, has_right = my_col > 0, my_col < n_cols - 1
    h_refs, l_refs, r_refs = (ha, hb), (left_a, left_b), (right_a, right_b)

    def mask(index):
        return mask_ref[index] > 0

    even, low_half = mask(0), mask(1)
    lane_first, lane_last = mask(2), mask(3)
    second = mask(4)
    bits = [mask(5 + level) for level in range(5)]

    def copy(src, dst, ssem, rsem, drow, dcol):
        return pltpu.make_async_remote_copy(src_ref=src, dst_ref=dst, send_sem=ssem, recv_sem=rsem,
                                            device_id={"rows": my_row + drow, "cols": my_col + dcol}, device_id_type=MESH)

    def col_copy(par, side, group):
        cards = pl.ds(card_from[group], len(GROUPS[group]))
        return copy(col_out.at[par, side, cards], col_in.at[par, side, cards], col_ssem.at[par, side, group],
                    col_rsem.at[par, side, group], 0, 1 if side == 0 else -1)

    def row_copy(par, side):
        return copy(row_out.at[par, side], row_in.at[par, side], row_ssem.at[par, side], row_rsem.at[par, side],
                    1 if side == 0 else -1, 0)

    def diag_copy(par, slot):
        return copy(col_out.at[par, slot % 2, 0], diag_in.at[par, slot], diag_ssem.at[par, slot],
                    diag_rsem.at[par, slot], 1 if slot < 2 else -1, 1 if slot % 2 == 0 else -1)

    col_to, col_from = (has_right, has_left), (has_left, has_right)
    row_to, row_from = (has_down, has_up), (has_up, has_down)
    diag_to = tuple((has_down if s < 2 else has_up) & col_to[s % 2] for s in range(4))
    diag_from = tuple((has_up if s < 2 else has_down) & col_from[s % 2] for s in range(4))

    def when(condition, transfers, method):
        @pl.when(condition)
        def _():
            for transfer in transfers:
                getattr(transfer, method)()

    def each_sent(par, group, condition, method):
        for side in range(2):
            when(col_to[side] & condition, [col_copy(par, side, group)], method)
        if group == 0:
            for side in range(2):
                when(row_to[side] & condition, [row_copy(par, side)], method)
            for slot in range(4):
                when(diag_to[slot] & condition, [diag_copy(par, slot)], method)

    def wait_for(par, group):
        for side in range(2):
            when(col_from[side], [col_copy(par, side, group)], "wait_recv")
        if group == 0:
            for side in range(2):
                when(row_from[side], [row_copy(par, side)], "wait_recv")
            for slot in range(4):
                when(diag_from[slot], [diag_copy(par, slot)], "wait_recv")

    def join(vectors, level):
        while len(vectors) > 1:
            pairs = [vectors[i:i + 2] for i in range(0, len(vectors), 2)]
            vectors = [jnp.where(bits[level], *pair) if len(pair) == 2 else pair[0] for pair in pairs]
            level += 1
        return vectors[0]

    def pack(parts, start):
        quads = [join([parts[i]] + [pltpu.roll(parts[i + j], 2 * j, 1) for j in range(1, 4)], 0) for i in range(0, len(parts), 4)]
        return [join([pltpu.roll(quad, (shift_by + 2 * start + 8 * i) % LANES, 1) for i, quad in enumerate(quads)], 2)
                for shift_by in (65, 63)]

    def shift(cells, message, amount):
        halo = pltpu.roll(message, amount % LANES, 1)
        return (jnp.where(lane_first, halo, pltpu.roll(cells, 1, 1)), jnp.where(lane_last, halo, pltpu.roll(cells, LANES - 1, 1)))

    def shifted(par, row, message, rolls):
        for g in range(groups):
            place = pl.ds(row * chan + 16 * g, 16)
            l_refs[par][place, :], r_refs[par][place, :] = shift(h_refs[par][place, :], message, rolls[g])

    def col_message(par, group):
        return jnp.where(even, col_in[par, 0, group], col_in[par, 1, group])

    def patch(par, chunks, edge):
        for chunk in chunks:
            message = col_message(par, home[chunk])
            for q in range(per):
                shifted(par, chunk * per + q + 1, message, [-2 * (base[chunk] + q * groups + g) for g in range(groups)])
        if edge is not None:
            side = 0 if edge == first else 1
            diag = jnp.where(even, diag_in[par, 2 * side], diag_in[par, 2 * side + 1])
            beside = col_message(par, 0)
            start = base[last] + (per - 1) * groups if edge == first else base[first]
            row = 0 if edge == first else half + 1
            for g in range(groups):
                place = slice(16 * g, 16 * (g + 1))
                mine, theirs = row_out[par, side, place, :], row_in[par, side, place, :]
                joined = jnp.where(low_half, theirs, mine) if edge == first else jnp.where(low_half, mine, theirs)
                h_refs[par][pl.ds(row * chan + 16 * g, 16), :] = joined
            message = jnp.where(second, diag, beside) if edge == first else jnp.where(second, beside, diag)
            shifted(par, row, message, [64 - 2 * (start + g) for g in range(groups)])

    def publish(par, chunk):
        parts = [h_refs[par][pl.ds((chunk * per + s // groups + 1) * chan + 16 * (s % groups), 16), :] for s in range(slots)]
        packed = pack(parts, base[chunk])
        card = home[chunk]
        for side in range(2):
            if chunk == members[card][-1]:
                earlier = [pieces[side, other] for other in members[card][:-1]]
                col_out[par, side, card] = join(earlier + [packed[side]], slots.bit_length() - 1)
            else:
                pieces[side, chunk] = packed[side]
        if chunk in (first, last):
            side = 0 if chunk == last else 1
            row = half if chunk == last else 1
            for g in range(groups):
                row_out[par, side, 16 * g:16 * (g + 1), :] = pltpu.roll(h_refs[par][pl.ds(row * chan + 16 * g, 16), :], 64, 1)

    frame_groups = fr_ref.shape[0]

    def frame_copies():
        for side in range(2):
            yield col_to[side], col_from[side], copy(f_col_out.at[side], f_col_in.at[side], f_ssem.at[side], f_rsem.at[side],
                                                     0, 1 if side == 0 else -1)
        for side in range(2):
            yield row_to[side], row_from[side], copy(f_row_out.at[side], f_row_in.at[side], f_ssem.at[2 + side],
                                                     f_rsem.at[2 + side], 1 if side == 0 else -1, 0)
        for slot in range(4):
            yield diag_to[slot], diag_from[slot], copy(f_col_out.at[slot % 2], f_diag_in.at[slot], f_ssem.at[4 + slot],
                                                       f_rsem.at[4 + slot], 1 if slot < 2 else -1, 1 if slot % 2 == 0 else -1)

    def send_frames():
        def build(tg, carry):
            f_mid[tg, 16:16 * (half + 1), :] = fr_ref[tg]
            f_col_out[0, tg], f_col_out[1, tg] = pack([fr_ref[tg, 16 * k:16 * (k + 1), :] for k in range(half)], 0)
            f_row_out[0, tg] = pltpu.roll(fr_ref[tg, 16 * (half - 1):16 * half, :], 64, 1)
            f_row_out[1, tg] = pltpu.roll(fr_ref[tg, 0:16, :], 64, 1)
            return carry

        lax.fori_loop(0, frame_groups, build, 0)
        for to, _, transfer in frame_copies():
            pl.when(to)(transfer.start)

    def receive_frames():
        for _, source, transfer in frame_copies():
            pl.when(source)(transfer.wait_recv)

        def place(tg, carry):
            message = jnp.where(even, f_col_in[0, tg], f_col_in[1, tg])
            above = jnp.where(even, f_diag_in[0, tg], f_diag_in[1, tg])
            below = jnp.where(even, f_diag_in[2, tg], f_diag_in[3, tg])
            rows = [(0, jnp.where(low_half, f_row_in[0, tg], f_row_out[0, tg]), jnp.where(second, above, message), 64 - 2 * (half - 1))]
            rows += [(k + 1, fr_ref[tg, 16 * k:16 * (k + 1), :], message, -2 * k) for k in range(half)]
            rows += [(half + 1, jnp.where(low_half, f_row_out[1, tg], f_row_in[1, tg]), jnp.where(second, message, below), 64)]
            for row, cells, beside, amount in rows:
                there = slice(16 * row, 16 * (row + 1))
                if row in (0, half + 1):
                    f_mid[tg, there, :] = cells
                f_left[tg, there, :], f_right[tg, there, :] = shift(cells, beside, amount)
            return carry

        lax.fori_loop(0, frame_groups, place, 0)
        for to, _, transfer in frame_copies():
            pl.when(to)(transfer.wait_send)

    def multiply(par, t, chunk, slot):
        blocks = []
        for q in range(per):
            place = pl.ds((chunk * per + q) * chan, 3 * chan)
            there = pl.ds((chunk * per + q) * 16, 48)
            frame = [f[lax.div(t, 4), there, :] for f in (f_left, f_mid, f_right)]
            blocks.append(jnp.concatenate([l_refs[par][place, :], h_refs[par][place, :], r_refs[par][place, :]] + frame, axis=0))
        gates[slot] = jnp.dot(w_ref[lax.rem(t, 4)], jnp.concatenate(blocks, axis=1), preferred_element_type=F32)

    def sigmoid(x):
        return 0.5 * jnp.tanh(0.5 * x) + 0.5

    def update(par, chunk, slot):
        for q in range(per):
            pre = [gates[slot, pl.ds(b * chan, chan), q * LANES:(q + 1) * LANES] + bias_ref[pl.ds(b * chan, chan), :]
                   for b in range(4)]
            place = pl.ds((chunk * per + q) * chan, chan)
            c_next = sigmoid(pre[1]) * c_ref[place, :] + sigmoid(pre[0]) * jnp.tanh(pre[3])
            c_ref[place, :] = c_next
            h_refs[par][pl.ds((chunk * per + q + 1) * chan, chan), :] = (sigmoid(pre[2]) * jnp.tanh(c_next)).astype(BF16)

    def out_copy(par, t):
        return pltpu.make_async_copy(h_refs[par].at[pl.ds(chan, half * chan), :], out_ref.at[t], out_sem.at[par])

    needs, seen = [], set()
    for chunk in order:
        chunks, edge = [], None
        for near in (chunk - 1, chunk, chunk + 1):
            if 0 <= near < n_chunks and near not in seen:
                seen.add(near)
                chunks.append(near)
        if chunk in (first, last):
            edge = chunk
        needs.append((chunks, edge))
    waits, waited = [], set()
    for chunks, edge in needs:
        which = {group_of[chunk] for chunk in chunks} | ({0} if edge is not None else set())
        waits.append(sorted(which - waited))
        waited |= which

    for par in range(2):
        col_in[par] = jnp.zeros(col_in.shape[1:], BF16)
        row_in[par] = jnp.zeros(row_in.shape[1:], BF16)
        diag_in[par] = jnp.zeros(diag_in.shape[1:], BF16)
    for ref in (f_col_in, f_row_in, f_diag_in):
        ref[...] = jnp.zeros(ref.shape, BF16)
    barrier = pltpu.get_barrier_semaphore()
    count = jnp.int32(0)
    for drow in (-1, 0, 1):
        for dcol in (-1, 0, 1):
            if (drow, dcol) == (0, 0):
                continue
            there = jnp.bool_(True)
            if drow:
                there = there & (has_down if drow > 0 else has_up)
            if dcol:
                there = there & (has_right if dcol > 0 else has_left)

            @pl.when(there)
            def _():
                pl.semaphore_signal(barrier, inc=1, device_id={"rows": my_row + drow, "cols": my_col + dcol}, device_id_type=MESH)
            count = count + there.astype(jnp.int32)
    pl.semaphore_wait(barrier, count)

    send_frames()
    for chunk in order:
        for k in range(chunk * per, (chunk + 1) * per):
            ha[pl.ds((k + 1) * chan, chan), :] = jnp.concatenate([h0_ref[k], h0_ref[k + half]], axis=0).T
        publish(0, chunk)
        if chunk in closing:
            each_sent(0, closing[chunk], True, "start")
    for k in range(half):
        c_ref[pl.ds(k * chan, chan), :] = jnp.concatenate([c0_ref[k], c0_ref[k + half]], axis=0).T
    receive_frames()

    def step(t, par, old):
        live = t < steps - 1

        @pl.when(old)
        def _():
            out_copy(1 - par, t - 2).wait()
        for group in range(len(GROUPS)):
            each_sent(1 - par, group, t > 0, "wait_send")
        for group in waits[0]:
            wait_for(par, group)
        patch(par, *needs[0])

        def finish(i):
            chunk = order[i]
            update(1 - par, chunk, i % 2)
            publish(1 - par, chunk)
            if chunk in closing:
                each_sent(1 - par, closing[chunk], live, "start")

        for i, chunk in enumerate(order):
            if i + 1 < n_chunks:
                for group in waits[i + 1]:
                    wait_for(par, group)
            multiply(par, t, chunk, i % 2)
            if i + 1 < n_chunks:
                patch(par, *needs[i + 1])
            if i > 0:
                finish(i - 1)
        finish(n_chunks - 1)
        out_copy(1 - par, t).start()

    def two_steps(i, carry):
        step(2 * i, 0, i > 0)
        step(2 * i + 1, 1, i > 0)
        return carry

    lax.fori_loop(0, steps // 2, two_steps, 0)
    for group in range(len(GROUPS)):
        each_sent(1, group, True, "wait_send")
    for k in range(half):
        cells = c_ref[pl.ds(k * chan, chan), :].T
        c_out_ref[k], c_out_ref[k + half] = cells[:LANES // 2], cells[LANES // 2:]
    out_copy(1, steps - 2).wait()
    out_copy(0, steps - 1).wait()


def lane_masks():
    lane = np.arange(LANES)
    even, slot = lane % 2 == 0, (lane + 1) // 2 % 32
    second = np.where(even, lane >= 64, (lane < 62) | (lane == 127))
    rows = [even, lane < 64, lane % 64 == 0, lane % 64 == 63, second] + [(slot >> level) % 2 == 0 for level in range(5)]
    return jnp.asarray(np.broadcast_to(np.stack(rows)[:, None, :], (len(rows), 16, LANES)).astype(np.float32), BF16)


def untile_kernel(x_ref, o_ref):
    half, chan = o_ref.shape[1] // 2, o_ref.shape[3]
    for t in range(o_ref.shape[0]):
        for k in range(half):
            cells = x_ref[t, pl.ds(k * chan, chan), :].T
            o_ref[t, k] = cells[:LANES // 2]
            o_ref[t, k + half] = cells[LANES // 2:]


N_CHUNKS = 16
GROUPS = ((3, 3, 3), (4, 3))
UNTILE = 4


def solution(mesh):
    n_rows, n_cols = mesh.shape["rows"], mesh.shape["cols"]
    seq_spec = P(None, "dp", "rows", "cols", None)
    state_spec = P("dp", "rows", "cols", None)

    def local_run(frames, w_in, w_rec, gate_bias, h_init, c_init):
        steps, batch, height, width, c_in = frames.shape
        chan = h_init.shape[-1]
        half = height // 2
        assert batch == 1 and width == 64 and chan == 64 and c_in == 4 and steps % 2 == 0
        assert steps % 4 == 0 and half == 32
        per = half // N_CHUNKS
        gates_n = w_rec.shape[-1]
        parts = frames.reshape(steps // 4, 4, 2, half, width, c_in).transpose(0, 3, 1, 5, 2, 4)
        parts = parts.reshape(steps // 4, half * 16, LANES)
        pick = jnp.eye(4, dtype=BF16)[:, None, None, :, None, None]
        w_x = (pick * w_in.transpose(1, 0, 2, 3)[None, :, :, None]).reshape(4, 9 * 16, gates_n)
        w_h = jnp.broadcast_to(w_rec.transpose(1, 0, 2, 3).reshape(1, 9 * chan, gates_n), (4, 9 * chan, gates_n))
        weights = jnp.concatenate([w_h, w_x], axis=1).transpose(0, 2, 1)
        bias = jnp.broadcast_to(gate_bias[:, None], (gates_n, LANES))

        vmem = pl.BlockSpec(memory_space=pltpu.VMEM)
        cells = pltpu.VMEM(((half + 2) * chan, LANES), BF16)
        dma = pltpu.SemaphoreType.DMA
        cards = sum(len(group) for group in GROUPS)
        cfg = (steps, half, chan, N_CHUNKS, n_rows, n_cols)
        hidden, c_last = pl.pallas_call(
            functools.partial(cell_kernel, cfg),
            out_shape=(jax.ShapeDtypeStruct((steps, half * chan, LANES), BF16), jax.ShapeDtypeStruct((height, width, chan), F32)),
            in_specs=[vmem] * 6,
            out_specs=(pl.BlockSpec(memory_space=pl.ANY), vmem),
            scratch_shapes=[cells] * 6 + [
                pltpu.VMEM((2, gates_n, per * LANES), F32), pltpu.VMEM((half * chan, LANES), F32),
            ] + [pltpu.VMEM((steps // 4, (half + 2) * 16, LANES), BF16)] * 3 + [
                pltpu.VMEM((2, steps // 4, 16, LANES), BF16), pltpu.VMEM((2, steps // 4, 16, LANES), BF16),
                pltpu.VMEM((2, steps // 4, 16, LANES), BF16), pltpu.VMEM((2, steps // 4, 16, LANES), BF16),
                pltpu.VMEM((4, steps // 4, 16, LANES), BF16), dma((8,)), dma((8,)),
                pltpu.VMEM((2, N_CHUNKS, 16, LANES), BF16),
                pltpu.VMEM((2, 2, cards, 16, LANES), BF16), pltpu.VMEM((2, 2, cards, 16, LANES), BF16),
                pltpu.VMEM((2, 2, chan, LANES), BF16), pltpu.VMEM((2, 2, chan, LANES), BF16),
                pltpu.VMEM((2, 4, 16, LANES), BF16),
                dma((2, 2, len(GROUPS))), dma((2, 2, len(GROUPS))), dma((2, 2)), dma((2, 2)), dma((2, 4)), dma((2, 4)), dma((2,)),
            ],
            compiler_params=pltpu.CompilerParams(collective_id=0, has_side_effects=True, vmem_limit_bytes=40 * 1024 * 1024),
        )(parts, weights, bias, h_init[0], c_init[0], lane_masks())

        hidden_seq = pl.pallas_call(
            untile_kernel,
            out_shape=jax.ShapeDtypeStruct((steps, height, width, chan), BF16),
            grid=(steps // UNTILE,),
            in_specs=[pl.BlockSpec((UNTILE, half * chan, LANES), lambda t: (t, 0, 0))],
            out_specs=pl.BlockSpec((UNTILE, height, width, chan), lambda t: (t, 0, 0, 0)),
        )(hidden)
        return hidden_seq[:, None], c_last[None]

    return jax.shard_map(local_run, mesh=mesh, in_specs=(seq_spec, P(), P(), P(), state_spec, state_spec),
                         out_specs=(seq_spec, state_spec), check_vma=False)
```

```python
import functools

import jax
import jax.numpy as jnp
import numpy as np
from jax import lax
from jax.experimental import pallas as pl
from jax.experimental.pallas import tpu as pltpu
from jax.sharding import PartitionSpec as P

MESH = pl.DeviceIdType.MESH
BF16, F32 = jnp.bfloat16, jnp.float32
LANES = 128


def chunk_order(n):
    order = [0]
    low, high = 1, n - 1
    while low <= high:
        order.append(low)
        if high != low:
            order.append(high)
        low, high = low + 1, high - 1
    return [(chunk + n // 2) % n for chunk in order]


def cell_kernel(cfg, fr_ref, w_ref, bias_ref, h0_ref, c0_ref, mask_ref, out_ref, c_out_ref,
                ha, hb, left_a, left_b, right_a, right_b, gates, c_ref, f_mid, f_left, f_right,
                f_col_out, f_col_in, f_row_out, f_row_in, f_diag_in, f_ssem, f_rsem,
                pieces, col_out, col_in, row_out, row_in, diag_in,
                col_ssem, col_rsem, row_ssem, row_rsem, diag_ssem, diag_rsem, out_sem):
    steps, half, chan, n_chunks, n_rows, n_cols = cfg
    per = half // n_chunks
    groups = chan // 16
    order = chunk_order(n_chunks)
    first, last = 0, n_chunks - 1
    slots = per * groups
    sizes = [size for group in GROUPS for size in group]
    ends = [sum(sizes[:i + 1]) for i in range(len(sizes))]
    home = {chunk: next(card for card, end in enumerate(ends) if place < end) for place, chunk in enumerate(order)}
    base = {chunk: slots * (place - ends[home[chunk]] + sizes[home[chunk]]) for place, chunk in enumerate(order)}
    members = [[chunk for chunk in order if home[chunk] == card] for card in range(len(sizes))]
    card_from = [sum(len(group) for group in GROUPS[:i]) for i in range(len(GROUPS) + 1)]
    group_of = {chunk: max(g for g in range(len(GROUPS)) if card_from[g] <= home[chunk]) for chunk in order}
    closing = {[chunk for chunk in order if group_of[chunk] == g][-1]: g for g in range(len(GROUPS))}
    assert sum(sizes) == n_chunks and max(sizes) * slots <= 32 and home[first] == home[last]
    my_row, my_col = lax.axis_index("rows"), lax.axis_index("cols")
    has_up, has_down = my_row > 0, my_row < n_rows - 1
    has_left, has_right = my_col > 0, my_col < n_cols - 1
    h_refs, l_refs, r_refs = (ha, hb), (left_a, left_b), (right_a, right_b)

    def mask(index):
        return mask_ref[index] > 0

    even, low_half = mask(0), mask(1)
    lane_first, lane_last = mask(2), mask(3)
    second = mask(4)
    bits = [mask(5 + level) for level in range(5)]

    def copy(src, dst, ssem, rsem, drow, dcol):
        return pltpu.make_async_remote_copy(src_ref=src, dst_ref=dst, send_sem=ssem, recv_sem=rsem,
                                            device_id={"rows": my_row + drow, "cols": my_col + dcol}, device_id_type=MESH)

    def col_copy(par, side, group):
        cards = pl.ds(card_from[group], len(GROUPS[group]))
        return copy(col_out.at[par, side, cards], col_in.at[par, side, cards], col_ssem.at[par, side, group],
                    col_rsem.at[par, side, group], 0, 1 if side == 0 else -1)

    edge_card, edge_group = home[first], group_of[first]

    def row_copy(par, side):
        return copy(row_out.at[par, side], row_in.at[par, side], row_ssem.at[par, side], row_rsem.at[par, side],
                    1 if side == 0 else -1, 0)

    def diag_copy(par, slot):
        return copy(col_out.at[par, slot % 2, edge_card], diag_in.at[par, slot], diag_ssem.at[par, slot],
                    diag_rsem.at[par, slot], 1 if slot < 2 else -1, 1 if slot % 2 == 0 else -1)

    col_to, col_from = (has_right, has_left), (has_left, has_right)
    row_to, row_from = (has_down, has_up), (has_up, has_down)
    diag_to = tuple((has_down if s < 2 else has_up) & col_to[s % 2] for s in range(4))
    diag_from = tuple((has_up if s < 2 else has_down) & col_from[s % 2] for s in range(4))

    def when(condition, transfers, method):
        @pl.when(condition)
        def _():
            for transfer in transfers:
                getattr(transfer, method)()

    def each_sent(par, group, condition, method):
        for side in range(2):
            when(col_to[side] & condition, [col_copy(par, side, group)], method)
        if group == edge_group:
            for side in range(2):
                when(row_to[side] & condition, [row_copy(par, side)], method)
            for slot in range(4):
                when(diag_to[slot] & condition, [diag_copy(par, slot)], method)

    def wait_for(par, group):
        for side in range(2):
            when(col_from[side], [col_copy(par, side, group)], "wait_recv")

    def wait_edges(par):
        for side in range(2):
            when(row_from[side], [row_copy(par, side)], "wait_recv")
        for slot in range(4):
            when(diag_from[slot], [diag_copy(par, slot)], "wait_recv")

    def join(vectors, level):
        while len(vectors) > 1:
            pairs = [vectors[i:i + 2] for i in range(0, len(vectors), 2)]
            vectors = [jnp.where(bits[level], *pair) if len(pair) == 2 else pair[0] for pair in pairs]
            level += 1
        return vectors[0]

    def pack(parts, start):
        quads = [join([parts[i]] + [pltpu.roll(parts[i + j], 2 * j, 1) for j in range(1, 4)], 0) for i in range(0, len(parts), 4)]
        return [join([pltpu.roll(quad, (shift_by + 2 * start + 8 * i) % LANES, 1) for i, quad in enumerate(quads)], 2)
                for shift_by in (65, 63)]

    def shift(cells, message, amount):
        halo = pltpu.roll(message, amount % LANES, 1)
        return (jnp.where(lane_first, halo, pltpu.roll(cells, 1, 1)), jnp.where(lane_last, halo, pltpu.roll(cells, LANES - 1, 1)))

    def shifted(par, row, message, rolls):
        for g in range(groups):
            place = pl.ds(row * chan + 16 * g, 16)
            l_refs[par][place, :], r_refs[par][place, :] = shift(h_refs[par][place, :], message, rolls[g])

    def col_message(par, group):
        return jnp.where(even, col_in[par, 0, group], col_in[par, 1, group])

    def patch(par, chunks, edge):
        for chunk in chunks:
            message = col_message(par, home[chunk])
            for q in range(per):
                shifted(par, chunk * per + q + 1, message, [-2 * (base[chunk] + q * groups + g) for g in range(groups)])
        if edge is not None:
            side = 0 if edge == first else 1
            diag = jnp.where(even, diag_in[par, 2 * side], diag_in[par, 2 * side + 1])
            beside = col_message(par, edge_card)
            start = base[last] + (per - 1) * groups if edge == first else base[first]
            row = 0 if edge == first else half + 1
            for g in range(groups):
                place = slice(16 * g, 16 * (g + 1))
                mine, theirs = row_out[par, side, place, :], row_in[par, side, place, :]
                joined = jnp.where(low_half, theirs, mine) if edge == first else jnp.where(low_half, mine, theirs)
                h_refs[par][pl.ds(row * chan + 16 * g, 16), :] = joined
            message = jnp.where(second, diag, beside) if edge == first else jnp.where(second, beside, diag)
            shifted(par, row, message, [64 - 2 * (start + g) for g in range(groups)])

    def publish(par, chunk):
        parts = [h_refs[par][pl.ds((chunk * per + s // groups + 1) * chan + 16 * (s % groups), 16), :] for s in range(slots)]
        packed = pack(parts, base[chunk])
        card = home[chunk]
        for side in range(2):
            if chunk == members[card][-1]:
                earlier = [pieces[side, other] for other in members[card][:-1]]
                col_out[par, side, card] = join(earlier + [packed[side]], slots.bit_length() - 1)
            else:
                pieces[side, chunk] = packed[side]
        if chunk in (first, last):
            side = 0 if chunk == last else 1
            row = half if chunk == last else 1
            for g in range(groups):
                row_out[par, side, 16 * g:16 * (g + 1), :] = pltpu.roll(h_refs[par][pl.ds(row * chan + 16 * g, 16), :], 64, 1)

    frame_groups = fr_ref.shape[0]

    def frame_copies():
        for side in range(2):
            yield col_to[side], col_from[side], copy(f_col_out.at[side], f_col_in.at[side], f_ssem.at[side], f_rsem.at[side],
                                                     0, 1 if side == 0 else -1)
        for side in range(2):
            yield row_to[side], row_from[side], copy(f_row_out.at[side], f_row_in.at[side], f_ssem.at[2 + side],
                                                     f_rsem.at[2 + side], 1 if side == 0 else -1, 0)
        for slot in range(4):
            yield diag_to[slot], diag_from[slot], copy(f_col_out.at[slot % 2], f_diag_in.at[slot], f_ssem.at[4 + slot],
                                                       f_rsem.at[4 + slot], 1 if slot < 2 else -1, 1 if slot % 2 == 0 else -1)

    def send_frames():
        def build(tg, carry):
            f_mid[tg, 16:16 * (half + 1), :] = fr_ref[tg]
            f_col_out[0, tg], f_col_out[1, tg] = pack([fr_ref[tg, 16 * k:16 * (k + 1), :] for k in range(half)], 0)
            f_row_out[0, tg] = pltpu.roll(fr_ref[tg, 16 * (half - 1):16 * half, :], 64, 1)
            f_row_out[1, tg] = pltpu.roll(fr_ref[tg, 0:16, :], 64, 1)
            return carry

        lax.fori_loop(0, frame_groups, build, 0)
        for to, _, transfer in frame_copies():
            pl.when(to)(transfer.start)

    def receive_frames():
        for _, source, transfer in frame_copies():
            pl.when(source)(transfer.wait_recv)

        def place(tg, carry):
            message = jnp.where(even, f_col_in[0, tg], f_col_in[1, tg])
            above = jnp.where(even, f_diag_in[0, tg], f_diag_in[1, tg])
            below = jnp.where(even, f_diag_in[2, tg], f_diag_in[3, tg])
            rows = [(0, jnp.where(low_half, f_row_in[0, tg], f_row_out[0, tg]), jnp.where(second, above, message), 64 - 2 * (half - 1))]
            rows += [(k + 1, fr_ref[tg, 16 * k:16 * (k + 1), :], message, -2 * k) for k in range(half)]
            rows += [(half + 1, jnp.where(low_half, f_row_out[1, tg], f_row_in[1, tg]), jnp.where(second, message, below), 64)]
            for row, cells, beside, amount in rows:
                there = slice(16 * row, 16 * (row + 1))
                if row in (0, half + 1):
                    f_mid[tg, there, :] = cells
                f_left[tg, there, :], f_right[tg, there, :] = shift(cells, beside, amount)
            return carry

        lax.fori_loop(0, frame_groups, place, 0)
        for to, _, transfer in frame_copies():
            pl.when(to)(transfer.wait_send)

    def multiply(par, t, chunk, slot):
        blocks = []
        for q in range(per):
            place = pl.ds((chunk * per + q) * chan, 3 * chan)
            there = pl.ds((chunk * per + q) * 16, 48)
            frame = [f[lax.div(t, 4), there, :] for f in (f_left, f_mid, f_right)]
            blocks.append(jnp.concatenate([l_refs[par][place, :], h_refs[par][place, :], r_refs[par][place, :]] + frame, axis=0))
        gates[slot] = jnp.dot(w_ref[lax.rem(t, 4)], jnp.concatenate(blocks, axis=1), preferred_element_type=F32)

    def sigmoid(x):
        return 0.5 * jnp.tanh(0.5 * x) + 0.5

    def update(par, chunk, slot):
        for q in range(per):
            pre = [gates[slot, pl.ds(b * chan, chan), q * LANES:(q + 1) * LANES] + bias_ref[pl.ds(b * chan, chan), :]
                   for b in range(4)]
            place = pl.ds((chunk * per + q) * chan, chan)
            c_next = sigmoid(pre[1]) * c_ref[place, :] + sigmoid(pre[0]) * jnp.tanh(pre[3])
            c_ref[place, :] = c_next
            h_refs[par][pl.ds((chunk * per + q + 1) * chan, chan), :] = (sigmoid(pre[2]) * jnp.tanh(c_next)).astype(BF16)

    def out_copy(par, t):
        return pltpu.make_async_copy(h_refs[par].at[pl.ds(chan, half * chan), :], out_ref.at[t], out_sem.at[par])

    needs, seen = [], set()
    for chunk in order:
        chunks, edge = [], None
        for near in (chunk - 1, chunk, chunk + 1):
            if 0 <= near < n_chunks and near not in seen:
                seen.add(near)
                chunks.append(near)
        if chunk in (first, last):
            edge = chunk
        needs.append((chunks, edge))
    waits, waited = [], set()
    for chunks, edge in needs:
        which = {group_of[chunk] for chunk in chunks} | ({edge_group} if edge is not None else set())
        waits.append(sorted(which - waited))
        waited |= which

    for par in range(2):
        col_in[par] = jnp.zeros(col_in.shape[1:], BF16)
        row_in[par] = jnp.zeros(row_in.shape[1:], BF16)
        diag_in[par] = jnp.zeros(diag_in.shape[1:], BF16)
    for ref in (f_col_in, f_row_in, f_diag_in):
        ref[...] = jnp.zeros(ref.shape, BF16)
    barrier = pltpu.get_barrier_semaphore()
    count = jnp.int32(0)
    for drow in (-1, 0, 1):
        for dcol in (-1, 0, 1):
            if (drow, dcol) == (0, 0):
                continue
            there = jnp.bool_(True)
            if drow:
                there = there & (has_down if drow > 0 else has_up)
            if dcol:
                there = there & (has_right if dcol > 0 else has_left)

            @pl.when(there)
            def _():
                pl.semaphore_signal(barrier, inc=1, device_id={"rows": my_row + drow, "cols": my_col + dcol}, device_id_type=MESH)
            count = count + there.astype(jnp.int32)
    pl.semaphore_wait(barrier, count)

    send_frames()
    for chunk in order:
        for k in range(chunk * per, (chunk + 1) * per):
            ha[pl.ds((k + 1) * chan, chan), :] = jnp.concatenate([h0_ref[k], h0_ref[k + half]], axis=0).T
        publish(0, chunk)
        if chunk in closing:
            each_sent(0, closing[chunk], True, "start")
    for k in range(half):
        c_ref[pl.ds(k * chan, chan), :] = jnp.concatenate([c0_ref[k], c0_ref[k + half]], axis=0).T
    receive_frames()

    def step(t, par, old):
        live = t < steps - 1

        @pl.when(old)
        def _():
            out_copy(1 - par, t - 2).wait()
        for group in range(len(GROUPS)):
            each_sent(1 - par, group, t > 0, "wait_send")
        for group in waits[0]:
            wait_for(par, group)
        patch(par, *needs[0])

        def finish(i):
            chunk = order[i]
            update(1 - par, chunk, i % 2)
            publish(1 - par, chunk)
            if chunk in closing:
                each_sent(1 - par, closing[chunk], live, "start")
                if closing[chunk] == 0:
                    wait_edges(par)

        for i, chunk in enumerate(order):
            if i + 1 < n_chunks:
                for group in waits[i + 1]:
                    wait_for(par, group)
            multiply(par, t, chunk, i % 2)
            if i + 1 < n_chunks:
                patch(par, *needs[i + 1])
            if i > 0:
                finish(i - 1)
        finish(n_chunks - 1)
        out_copy(1 - par, t).start()

    def two_steps(i, carry):
        step(2 * i, 0, i > 0)
        step(2 * i + 1, 1, i > 0)
        return carry

    lax.fori_loop(0, steps // 2, two_steps, 0)
    for group in range(len(GROUPS)):
        each_sent(1, group, True, "wait_send")
    for k in range(half):
        cells = c_ref[pl.ds(k * chan, chan), :].T
        c_out_ref[k], c_out_ref[k + half] = cells[:LANES // 2], cells[LANES // 2:]
    out_copy(1, steps - 2).wait()
    out_copy(0, steps - 1).wait()


def lane_masks():
    lane = np.arange(LANES)
    even, slot = lane % 2 == 0, (lane + 1) // 2 % 32
    second = np.where(even, lane >= 64, (lane < 62) | (lane == 127))
    rows = [even, lane < 64, lane % 64 == 0, lane % 64 == 63, second] + [(slot >> level) % 2 == 0 for level in range(5)]
    return jnp.asarray(np.broadcast_to(np.stack(rows)[:, None, :], (len(rows), 16, LANES)).astype(np.float32), BF16)


def untile_kernel(x_ref, o_ref):
    half, chan = o_ref.shape[1] // 2, o_ref.shape[3]
    for t in range(o_ref.shape[0]):
        for k in range(half):
            cells = x_ref[t, pl.ds(k * chan, chan), :].T
            o_ref[t, k] = cells[:LANES // 2]
            o_ref[t, k + half] = cells[LANES // 2:]


N_CHUNKS = 16
GROUPS = ((3, 3, 3), (3, 4))
UNTILE = 4


def solution(mesh):
    n_rows, n_cols = mesh.shape["rows"], mesh.shape["cols"]
    seq_spec = P(None, "dp", "rows", "cols", None)
    state_spec = P("dp", "rows", "cols", None)

    def local_run(frames, w_in, w_rec, gate_bias, h_init, c_init):
        steps, batch, height, width, c_in = frames.shape
        chan = h_init.shape[-1]
        half = height // 2
        assert batch == 1 and width == 64 and chan == 64 and c_in == 4 and steps % 2 == 0
        assert steps % 4 == 0 and half == 32
        per = half // N_CHUNKS
        gates_n = w_rec.shape[-1]
        parts = frames.reshape(steps // 4, 4, 2, half, width, c_in).transpose(0, 3, 1, 5, 2, 4)
        parts = parts.reshape(steps // 4, half * 16, LANES)
        pick = jnp.eye(4, dtype=BF16)[:, None, None, :, None, None]
        w_x = (pick * w_in.transpose(1, 0, 2, 3)[None, :, :, None]).reshape(4, 9 * 16, gates_n)
        w_h = jnp.broadcast_to(w_rec.transpose(1, 0, 2, 3).reshape(1, 9 * chan, gates_n), (4, 9 * chan, gates_n))
        weights = jnp.concatenate([w_h, w_x], axis=1).transpose(0, 2, 1)
        bias = jnp.broadcast_to(gate_bias[:, None], (gates_n, LANES))

        vmem = pl.BlockSpec(memory_space=pltpu.VMEM)
        cells = pltpu.VMEM(((half + 2) * chan, LANES), BF16)
        dma = pltpu.SemaphoreType.DMA
        cards = sum(len(group) for group in GROUPS)
        cfg = (steps, half, chan, N_CHUNKS, n_rows, n_cols)
        hidden, c_last = pl.pallas_call(
            functools.partial(cell_kernel, cfg),
            out_shape=(jax.ShapeDtypeStruct((steps, half * chan, LANES), BF16), jax.ShapeDtypeStruct((height, width, chan), F32)),
            in_specs=[vmem] * 6,
            out_specs=(pl.BlockSpec(memory_space=pl.ANY), vmem),
            scratch_shapes=[cells] * 6 + [
                pltpu.VMEM((2, gates_n, per * LANES), F32), pltpu.VMEM((half * chan, LANES), F32),
            ] + [pltpu.VMEM((steps // 4, (half + 2) * 16, LANES), BF16)] * 3 + [
                pltpu.VMEM((2, steps // 4, 16, LANES), BF16), pltpu.VMEM((2, steps // 4, 16, LANES), BF16),
                pltpu.VMEM((2, steps // 4, 16, LANES), BF16), pltpu.VMEM((2, steps // 4, 16, LANES), BF16),
                pltpu.VMEM((4, steps // 4, 16, LANES), BF16), dma((8,)), dma((8,)),
                pltpu.VMEM((2, N_CHUNKS, 16, LANES), BF16),
                pltpu.VMEM((2, 2, cards, 16, LANES), BF16), pltpu.VMEM((2, 2, cards, 16, LANES), BF16),
                pltpu.VMEM((2, 2, chan, LANES), BF16), pltpu.VMEM((2, 2, chan, LANES), BF16),
                pltpu.VMEM((2, 4, 16, LANES), BF16),
                dma((2, 2, len(GROUPS))), dma((2, 2, len(GROUPS))), dma((2, 2)), dma((2, 2)), dma((2, 4)), dma((2, 4)), dma((2,)),
            ],
            compiler_params=pltpu.CompilerParams(collective_id=0, has_side_effects=True, vmem_limit_bytes=40 * 1024 * 1024),
        )(parts, weights, bias, h_init[0], c_init[0], lane_masks())

        hidden_seq = pl.pallas_call(
            untile_kernel,
            out_shape=jax.ShapeDtypeStruct((steps, height, width, chan), BF16),
            grid=(steps // UNTILE,),
            in_specs=[pl.BlockSpec((UNTILE, half * chan, LANES), lambda t: (t, 0, 0))],
            out_specs=pl.BlockSpec((UNTILE, height, width, chan), lambda t: (t, 0, 0, 0)),
        )(hidden)
        return hidden_seq[:, None], c_last[None]

    return jax.shard_map(local_run, mesh=mesh, in_specs=(seq_spec, P(), P(), P(), state_spec, state_spec),
                         out_specs=(seq_spec, state_spec), check_vma=False)
```
